32 devices in a mesh: blk: 32 (over z, y, x, core).
Axes of the slice: x: 2, y: 2, z: 4, core: 2. Of those that a mesh axis runs over, the one named last changes fastest.
Arguments:
- queries: bfloat16 [2048, 4096], P('blk'), may hold values from -200 to 200
- keys: bfloat16 [2048, 2048], P('blk'), may hold values from -8 to 8
- values: bfloat16 [2048, 2048], P('blk'), may hold values from -6 to 6
- doc_start: int32 [2048], P('blk'), may hold values from 0 to 2047, as said below
Outputs:
- attended: bfloat16 [2048, 4096], P('blk')
The draws below stay inside these ranges and needn't reach their ends.
Inputs may be any that keep to these rules, and one draw needn't show every extreme that they name: doc_start[i] is the first position of token i's document: nondecreasing, at most i, doc_start[doc_start[i]] = doc_start[i], and position 0 starts a document.
All inputs are finite; a program needn't handle non-finite values.
Results may differ from the reference program's by a relative error of at most 0.0034.
Values may be sent and summed in bfloat16 or wider, within the bound.
A program may use at most 64 MiB of HBM per device.

```python
import jax
import jax.numpy as jnp
from jax import lax

HEADS = 16
KV_HEADS = 8
HD = 256
TOK_DEV = 64
HOPS = 4
GROUP = 2
TOKENS = 2048


def drawn_pair(key):
    base = jax.random.fold_in(key, 11)
    key_q, key_k = jax.random.split(base, 2)
    key_vectors = jax.random.normal(key_k, (TOKENS, KV_HEADS * HD), jnp.float32)
    query_vectors = jax.random.normal(key_q, (TOKENS, HEADS * HD), jnp.float32)
    query_vectors = jnp.clip(query_vectors, -5.0, 5.0)
    key_vectors = jnp.clip(key_vectors, -5.0, 5.0)
    return (query_vectors, key_vectors)


def draw_queries(key, part):
    query_vectors, key_vectors = drawn_pair(key)
    return query_vectors.astype(jnp.bfloat16)


def draw_keys(key, part):
    query_vectors, key_vectors = drawn_pair(key)
    return key_vectors.astype(jnp.bfloat16)


def draw_doc_start(key, part):
    base = jax.random.fold_in(key, 23)
    key_kind, key_cut = jax.random.split(base)
    nblocks = TOKENS // TOK_DEV
    longer = jax.random.randint(key_kind, (nblocks,), 0, 2)
    period = jnp.where(longer == 1, 6 * TOK_DEV, 24).astype(jnp.int32)
    period = jnp.repeat(period, TOK_DEV)
    draws = jax.random.randint(key_cut, (TOKENS,), 0, 1 << 30)
    positions = jnp.arange(TOKENS, dtype=jnp.int32)
    boundary = (draws % period == 0) | (positions == 0)
    marks = jnp.where(boundary, positions, jnp.int32(0))
    return lax.cummax(marks, axis=0).astype(jnp.int32)


def block_scale(key, dims, cuts, low, top_value):
    level, own = 1.0, jax.random.fold_in(key, 6)
    for position, shards_of in cuts:
        heights = jnp.exp(jax.random.uniform(jax.random.fold_in(own, position), (shards_of,), jnp.float32, low / len(cuts), top_value / len(cuts)))
        level = level * jnp.repeat(heights, dims[position] // shards_of).reshape([-1 if axis == position else 1 for axis in range(len(dims))])
    return level


def bell_draw(own_key, extent, scale, reach, pieces=(), kind=jnp.bfloat16):
    drawn = jax.random.normal(own_key, extent, jnp.float32) * scale
    if len(pieces) > 0:
        drawn = block_scale(own_key, extent, pieces, -0.22, 0.18) * drawn
    return jnp.clip(drawn, min=-reach, max=reach).astype(kind)


def setup_inputs(seed: int = 0) -> dict:
    streams_of = jax.random.split(jax.random.key(seed), 5)
    return {
        "queries": draw_queries(jax.random.fold_in(streams_of[4], 71), 0),
        "keys": draw_keys(jax.random.fold_in(streams_of[4], 71), 0),
        "values": bell_draw(streams_of[2], (TOKENS, KV_HEADS * HD), 1.0, 6.0, ((0, 32),)),
        "doc_start": draw_doc_start(jax.random.fold_in(streams_of[4], 71), 0),
    }


def reference(queries, keys, values, doc_start):
    window = HOPS * TOK_DEV
    span = window + TOK_DEV
    key_pad = jnp.pad(keys, ((window, 0), (0, 0)))
    value_pad = jnp.pad(values, ((window, 0), (0, 0)))

    def one_block(index):
        start = (index * TOK_DEV).astype(jnp.int32)
        query_block = lax.dynamic_slice(queries, (start, jnp.int32(0)), (TOK_DEV, HEADS * HD))
        query_block = query_block.astype(jnp.float32).reshape(TOK_DEV, KV_HEADS, GROUP, HD)
        key_block = lax.dynamic_slice(key_pad, (start, jnp.int32(0)), (span, KV_HEADS * HD))
        key_block = key_block.astype(jnp.float32).reshape(span, KV_HEADS, HD)
        value_block = lax.dynamic_slice(value_pad, (start, jnp.int32(0)), (span, KV_HEADS * HD))
        value_block = value_block.astype(jnp.float32).reshape(span, KV_HEADS, HD)
        scores = jnp.einsum('qgrd,kgd->grqk', query_block, key_block) * 0.0625
        q_pos = start + jnp.arange(TOK_DEV, dtype=jnp.int32)
        k_pos = start - window + jnp.arange(span, dtype=jnp.int32)
        starts = lax.dynamic_slice(doc_start, (start,), (TOK_DEV,))
        allowed = (k_pos[None, :] <= q_pos[:, None]) & (q_pos[:, None] - k_pos[None, :] < window) & (k_pos[None, :] >= starts[:, None])
        scores = jnp.where(allowed, scores, jnp.float32(-1e30))
        top = jnp.max(scores, axis=-1, keepdims=True)
        expo = jnp.exp(scores - top)
        total = jnp.sum(expo, axis=-1)
        weights = lax.optimization_barrier(expo.astype(jnp.bfloat16)).astype(jnp.float32)
        mixed = jnp.einsum('grqk,kgd->qgrd', weights, value_block)
        mixed = mixed / jnp.transpose(total, (2, 0, 1))[..., None]
        return mixed.reshape(TOK_DEV, HEADS * HD).astype(jnp.bfloat16)

    blocks = lax.map(one_block, jnp.arange(TOKENS // TOK_DEV, dtype=jnp.int32))
    return blocks.reshape(TOKENS, HEADS * HD)
```

```python
import functools

import jax
import jax.numpy as jnp
from jax import lax
from jax.experimental import pallas as pl
from jax.experimental.pallas import tpu as pltpu
from jax.sharding import PartitionSpec as P

HD = 256
HOPS = 4
NEGATIVE = -1e30
MESH = pl.DeviceIdType.MESH


def kernel(
    n, q_hbm, k_hbm, v_hbm, doc_ref, out_ref,
    q_buf, kv, bias, q_sem, own_sem,
    y_send, y_recv, x_send, x_recv, o_send, o_recv, p_send, p_recv, pp_send, pp_recv,
):
    rows = q_hbm.shape[0]
    heads = k_hbm.shape[1] // HD
    groups = q_hbm.shape[1] // k_hbm.shape[1]
    window = HOPS * rows
    span = window + rows
    wide = groups * HD

    me = lax.axis_index("blk")
    core = lax.rem(me, 2)
    chip = me // 2
    odd = lax.rem(chip, 2)
    partner = me + 1 - 2 * core
    beside = me + 2 - 4 * odd
    has_far = me >= 4
    has_near = jnp.logical_or(odd == 1, has_far)
    sends_far = me + 4 < n
    far_to = lax.rem(me + 4, n)

    def slot(number):
        return pl.ds(pl.multiple_of(number * rows, rows), rows)

    def own_copy(h, which):
        src = (k_hbm, v_hbm)[which]
        columns = pl.ds(pl.multiple_of(h * HD, HD), HD)
        return pltpu.make_async_copy(
            src.at[:, columns], kv.at[h, which, slot(4 + core), :], own_sem.at[which, h]
        )

    def remote(h, source, target, send, recv, device):
        return pltpu.make_async_remote_copy(
            src_ref=kv.at[h, :, slot(source), :],
            dst_ref=kv.at[h, :, slot(target), :],
            send_sem=send.at[h],
            recv_sem=recv.at[h],
            device_id=(device,),
            device_id_type=MESH,
        )

    def far_copy(h):
        return remote(h, 4 + core, core, y_send, y_recv, far_to)

    def near_copy(h):
        return remote(h, core + 4 * (1 - odd), 2 + core, x_send, x_recv, beside)

    def share_own(h):
        return remote(h, 4, 4, o_send, o_recv, partner)

    def share_near(h):
        return remote(h, 2 + core, 2 + core, p_send, p_recv, partner)

    def near_shared(h):
        return remote(h, 3 - core, 3 - core, p_send, p_recv, partner)

    def share_far(h):
        return remote(h, 1, 1, pp_send, pp_recv, partner)

    def each_head(body):
        def step(h, carry):
            body(h)
            return carry

        lax.fori_loop(0, heads, step, 0)

    q_copy = pltpu.make_async_copy(q_hbm, q_buf, q_sem)

    def load(h):
        own_copy(h, 0).start()
        own_copy(h, 1).start()

    each_head(load)
    q_copy.start()

    barrier = pltpu.get_barrier_semaphore()

    def greet(device):
        pl.semaphore_signal(barrier, inc=1, device_id=(device,), device_id_type=MESH)

    greet(partner)
    greet(beside)

    @pl.when(sends_far)
    def _():
        greet(me + 4)

    @pl.when(has_far)
    def _():
        greet(me - 4)

    pl.semaphore_wait(barrier, 2 + jnp.where(sends_far, 1, 0) + jnp.where(has_far, 1, 0))

    def send(h):
        own_copy(h, 0).wait()
        own_copy(h, 1).wait()

        @pl.when(sends_far)
        def _():
            far_copy(h).start()

        @pl.when(odd == 0)
        def _():
            near_copy(h).start()

        @pl.when(core == 0)
        def _():
            share_own(h).start()

    each_head(send)

    @pl.when(me < 4)
    def _():
        def clear(h):
            kv[h, :, 0 : 2 * rows, :] = jnp.zeros((2, 2 * rows, HD), kv.dtype)

        each_head(clear)

    @pl.when(me < 2)
    def _():
        def clear(h):
            kv[h, :, 2 * rows : 4 * rows, :] = jnp.zeros((2, 2 * rows, HD), kv.dtype)

        each_head(clear)

    square_row = lax.broadcasted_iota(jnp.int32, (rows, rows), 0)
    square_col = lax.broadcasted_iota(jnp.int32, (rows, rows), 1)
    spread = jnp.broadcast_to(doc_ref[...], (rows, rows)).astype(jnp.float32)
    starts = jnp.sum(jnp.where(square_row == square_col, spread, 0.0), axis=1, keepdims=True)
    starts = starts.astype(jnp.int32)
    q_pos = me * rows + lax.broadcasted_iota(jnp.int32, (rows, span), 0)
    k_pos = (me - HOPS) * rows + lax.broadcasted_iota(jnp.int32, (rows, span), 1)
    allowed = (k_pos <= q_pos) & (q_pos - k_pos < window) & (k_pos >= starts)
    bias[...] = jnp.where(allowed, 0.0, NEGATIVE)
    q_copy.wait()

    def relay(h):
        @pl.when(has_far)
        def _():
            far_copy(h).wait_recv()

            @pl.when(odd == 1)
            def _():
                near_copy(h).start()

            @pl.when(core == 1)
            def _():
                share_far(h).start()

        @pl.when(has_near)
        def _():
            near_copy(h).wait_recv()
            share_near(h).start()

    def attend(h):
        @pl.when(has_near)
        def _():
            near_shared(h).wait_recv()

        @pl.when(jnp.logical_and(has_far, core == 0))
        def _():
            share_far(h).wait_recv()

        @pl.when(core == 1)
        def _():
            share_own(h).wait_recv()

        columns = pl.ds(pl.multiple_of(h * wide, wide), wide)
        query = q_buf[:, columns]
        query = jnp.concatenate(
            [query[:, g * HD : (g + 1) * HD] for g in range(groups)], axis=0
        )
        reach = pl.ds(pl.multiple_of(core * rows, rows), span)
        scores = lax.dot_general(
            query, kv[h, 0, reach, :], (((1,), (1,)), ((), ())),
            preferred_element_type=jnp.float32,
        ) * 0.0625
        hidden = jnp.concatenate([bias[...]] * groups, axis=0) < 0
        scores = jnp.where(hidden, NEGATIVE, scores)
        top = jnp.max(scores, axis=1, keepdims=True)
        expo = jnp.exp(scores - top)
        total = jnp.sum(expo, axis=1, keepdims=True)
        mixed = jnp.dot(
            expo.astype(jnp.bfloat16), kv[h, 1, reach, :],
            preferred_element_type=jnp.float32,
        )
        mixed = (mixed / total).astype(out_ref.dtype)
        out_ref[:, columns] = jnp.concatenate(
            [mixed[g * rows : (g + 1) * rows] for g in range(groups)], axis=1
        )

    def turn(h, carry):
        @pl.when(h < heads)
        def _():
            relay(h)

        @pl.when(h >= 1)
        def _():
            attend(h - 1)

        return carry

    lax.fori_loop(0, heads + 1, turn, 0)

    def drain(h):
        @pl.when(sends_far)
        def _():
            far_copy(h).wait_send()

        @pl.when(has_far)
        def _():
            @pl.when(core == 1)
            def _():
                share_far(h).wait_send()

        @pl.when(jnp.logical_or(odd == 0, has_far))
        def _():
            near_copy(h).wait_send()

        @pl.when(has_near)
        def _():
            share_near(h).wait_send()

        @pl.when(core == 0)
        def _():
            share_own(h).wait_send()

    each_head(drain)


def solution(mesh):
    n = mesh.shape["blk"]

    def per_device(queries, keys, values, doc_start):
        rows, columns = queries.shape
        heads = keys.shape[1] // HD
        span = (HOPS + 1) * rows
        remote_sems = [pltpu.SemaphoreType.DMA((heads,)) for _ in range(10)]
        return pl.pallas_call(
            functools.partial(kernel, n),
            out_shape=jax.ShapeDtypeStruct((rows, columns), jnp.bfloat16),
            in_specs=[pl.BlockSpec(memory_space=pl.ANY)] * 3
            + [pl.BlockSpec(memory_space=pltpu.VMEM)],
            out_specs=pl.BlockSpec(memory_space=pltpu.VMEM),
            scratch_shapes=[
                pltpu.VMEM((rows, columns), jnp.bfloat16),
                pltpu.VMEM((heads, 2, (HOPS + 2) * rows, HD), jnp.bfloat16),
                pltpu.VMEM((rows, span), jnp.float32),
                pltpu.SemaphoreType.DMA,
                pltpu.SemaphoreType.DMA((2, heads)),
            ]
            + remote_sems,
            compiler_params=pltpu.CompilerParams(collective_id=0, has_side_effects=True),
        )(queries, keys, values, doc_start.reshape(1, rows))

    return jax.shard_map(
        per_device,
        mesh=mesh,
        in_specs=(P("blk", None), P("blk", None), P("blk", None), P("blk")),
        out_specs=P("blk", None),
        check_vma=False,
    )
```

```python
import functools

import jax
import jax.numpy as jnp
from jax import lax
from jax.experimental import pallas as pl
from jax.experimental.pallas import tpu as pltpu
from jax.sharding import PartitionSpec as P

HD = 256
HOPS = 4
NEGATIVE = -1e30
FORWARD_AT = 2
MESH = pl.DeviceIdType.MESH


def kernel(
    n, q_hbm, k_hbm, v_hbm, doc_ref, out_ref,
    q_buf, kv, passing, passing_half, bias, q_sem, own_sem, half_sems, pass_send, pass_recv, onward_send, onward_recv,
    y_send, y_recv, x_send, x_recv, o_send, o_recv, p_send, p_recv, pp_send, pp_recv,
):
    rows = q_hbm.shape[0]
    heads = k_hbm.shape[1] // HD
    groups = q_hbm.shape[1] // k_hbm.shape[1]
    window = HOPS * rows
    span = window + rows
    wide = groups * HD

    me = lax.axis_index("blk")
    core = lax.rem(me, 2)
    chip = me // 2
    odd = lax.rem(chip, 2)
    partner = me + 1 - 2 * core
    beside = me + 2 - 4 * odd
    has_far = me >= 4
    has_near = jnp.logical_or(odd == 1, has_far)
    sends_far = me + 4 < n
    far_to = lax.rem(me + 4, n)

    def slot(number):
        return pl.ds(pl.multiple_of(number * rows, rows), rows)

    def own_copy(h, which):
        src = (k_hbm, v_hbm)[which]
        columns = pl.ds(pl.multiple_of(h * HD, HD), HD)
        return pltpu.make_async_copy(
            src.at[:, columns], kv.at[h, which, slot(4 + core), :], own_sem.at[which, h]
        )

    def remote(h, source, target, send, recv, device):
        return pltpu.make_async_remote_copy(
            src_ref=kv.at[h, :, slot(source), :],
            dst_ref=kv.at[h, :, slot(target), :],
            send_sem=send.at[h],
            recv_sem=recv.at[h],
            device_id=(device,),
            device_id_type=MESH,
        )

    def far_copy(h):
        return remote(h, 4 + core, core, y_send, y_recv, far_to)

    def near_copy(h):
        return remote(h, core + 4 * (1 - odd), 2 + core, x_send, x_recv, beside)

    last = heads - 2

    def odd_order(i):
        return jnp.where(i >= last, 2 * heads - 3 - i, i)

    def order(i):
        return jnp.where(odd == 1, odd_order(i), i)

    def pass_copy():
        return pltpu.make_async_remote_copy(
            src_ref=kv.at[last, :, slot(4 + core), :],
            dst_ref=passing,
            send_sem=pass_send,
            recv_sem=pass_recv,
            device_id=(beside,),
            device_id_type=MESH,
        )

    def half_pass():
        return pltpu.make_async_remote_copy(
            src_ref=kv.at[heads - 1, 1, slot(4 + core), :],
            dst_ref=passing_half,
            send_sem=half_sems.at[0],
            recv_sem=half_sems.at[1],
            device_id=(beside,),
            device_id_type=MESH,
        )

    def half_onward():
        return pltpu.make_async_remote_copy(
            src_ref=passing_half,
            dst_ref=kv.at[heads - 1, 1, slot(2 + core), :],
            send_sem=half_sems.at[2],
            recv_sem=half_sems.at[3],
            device_id=(far_to,),
            device_id_type=MESH,
        )

    def near_half():
        return pltpu.make_async_remote_copy(
            src_ref=kv.at[heads - 1, 0, slot(core + 4 * (1 - odd)), :],
            dst_ref=kv.at[heads - 1, 0, slot(2 + core), :],
            send_sem=half_sems.at[4],
            recv_sem=half_sems.at[5],
            device_id=(beside,),
            device_id_type=MESH,
        )

    def onward_copy():
        return pltpu.make_async_remote_copy(
            src_ref=passing,
            dst_ref=kv.at[last, :, slot(2 + core), :],
            send_sem=onward_send,
            recv_sem=onward_recv,
            device_id=(far_to,),
            device_id_type=MESH,
        )

    def share_own(h):
        return remote(h, 4, 4, o_send, o_recv, partner)

    def share_near(h):
        return remote(h, 2 + core, 2 + core, p_send, p_recv, partner)

    def near_shared(h):
        return remote(h, 3 - core, 3 - core, p_send, p_recv, partner)

    def share_far(h):
        return remote(h, 1, 1, pp_send, pp_recv, partner)

    def each_head(body):
        def step(h, carry):
            body(h)
            return carry

        lax.fori_loop(0, heads, step, 0)

    barrier = pltpu.get_barrier_semaphore()

    def greet(device):
        pl.semaphore_signal(barrier, inc=1, device_id=(device,), device_id_type=MESH)

    @pl.when(sends_far)
    def _():
        greet(me + 4)

    @pl.when(has_far)
    def _():
        greet(me - 4)

    greet(beside)
    greet(partner)

    q_copy = pltpu.make_async_copy(q_hbm, q_buf, q_sem)

    def load(h):
        own_copy(h, 0).start()
        own_copy(h, 1).start()

    each_head(load)
    q_copy.start()

    pl.semaphore_wait(barrier, 2 + jnp.where(sends_far, 1, 0) + jnp.where(has_far, 1, 0))

    passes = jnp.logical_and(sends_far, odd == 1)
    onward = jnp.logical_and(sends_far, odd == 0)
    takes = jnp.logical_and(has_far, odd == 0)

    def own_copy_wait(h):
        own_copy(h, 0).wait()
        own_copy(h, 1).wait()

    each_head(own_copy_wait)

    def send(i):
        h, near_head = order(i), odd_order(i)


        @pl.when(sends_far)
        def _():
            far_copy(h).start()

        @pl.when(odd == 0)
        def _():
            near_copy(near_head).start()

        @pl.when(core == 0)
        def _():
            share_own(h).start()

    each_head(send)

    @pl.when(passes)
    def _():
        pass_copy().start()
        half_pass().start()

    @pl.when(me < 4)
    def _():
        def clear(h):
            kv[h, :, 0 : 2 * rows, :] = jnp.zeros((2, 2 * rows, HD), kv.dtype)

        each_head(clear)

    @pl.when(me < 2)
    def _():
        def clear(h):
            kv[h, :, 2 * rows : 4 * rows, :] = jnp.zeros((2, 2 * rows, HD), kv.dtype)

        each_head(clear)

    square_row = lax.broadcasted_iota(jnp.int32, (rows, rows), 0)
    square_col = lax.broadcasted_iota(jnp.int32, (rows, rows), 1)
    spread = jnp.broadcast_to(doc_ref[...], (rows, rows)).astype(jnp.float32)
    starts = jnp.sum(jnp.where(square_row == square_col, spread, 0.0), axis=1, keepdims=True)
    starts = starts.astype(jnp.int32)
    q_pos = me * rows + lax.broadcasted_iota(jnp.int32, (rows, span), 0)
    k_pos = (me - HOPS) * rows + lax.broadcasted_iota(jnp.int32, (rows, span), 1)
    allowed = (k_pos <= q_pos) & (q_pos - k_pos < window) & (k_pos >= starts)
    bias[...] = jnp.where(allowed, 0.0, NEGATIVE)
    q_copy.wait()

    def relay(h):
        @pl.when(has_far)
        def _():
            far_copy(h).wait_recv()

            @pl.when(jnp.logical_and(odd == 1, h < last))
            def _():
                near_copy(h).start()

            @pl.when(jnp.logical_and(odd == 1, h > last))
            def _():
                near_half().start()

            @pl.when(core == 1)
            def _():
                share_far(h).start()

        @pl.when(has_near)
        def _():
            by_way = jnp.logical_and(takes, h == last)

            @pl.when(by_way)
            def _():
                onward_copy().wait_recv()

            by_halves = jnp.logical_and(takes, h > last)

            @pl.when(by_halves)
            def _():
                near_half().wait_recv()
                half_onward().wait_recv()

            @pl.when(jnp.logical_not(jnp.logical_or(by_way, by_halves)))
            def _():
                near_copy(h).wait_recv()

            share_near(h).start()

    def attend(h):
        @pl.when(has_near)
        def _():
            near_shared(h).wait_recv()

        @pl.when(jnp.logical_and(has_far, core == 0))
        def _():
            share_far(h).wait_recv()

        @pl.when(core == 1)
        def _():
            share_own(h).wait_recv()

        columns = pl.ds(pl.multiple_of(h * wide, wide), wide)
        query = q_buf[:, columns]
        query = jnp.concatenate(
            [query[:, g * HD : (g + 1) * HD] for g in range(groups)], axis=0
        )
        reach = pl.ds(pl.multiple_of(core * rows, rows), span)
        scores = lax.dot_general(
            query, kv[h, 0, reach, :], (((1,), (1,)), ((), ())),
            preferred_element_type=jnp.float32,
        ) * 0.0625
        hidden = jnp.concatenate([bias[...]] * groups, axis=0) < 0
        scores = jnp.where(hidden, NEGATIVE, scores)
        top = jnp.max(scores, axis=1, keepdims=True)
        expo = jnp.exp(scores - top)
        total = jnp.sum(expo, axis=1, keepdims=True)
        mixed = jnp.dot(
            expo.astype(jnp.bfloat16), kv[h, 1, reach, :],
            preferred_element_type=jnp.float32,
        )
        mixed = (mixed / total).astype(out_ref.dtype)
        out_ref[:, columns] = jnp.concatenate(
            [mixed[g * rows : (g + 1) * rows] for g in range(groups)], axis=1
        )

    def turn(h, carry):
        @pl.when(jnp.logical_and(onward, h == FORWARD_AT))
        def _():
            pass_copy().wait_recv()
            onward_copy().start()
            half_pass().wait_recv()
            half_onward().start()

        @pl.when(h < heads)
        def _():
            relay(order(h))

        @pl.when(h >= 1)
        def _():
            attend(order(h - 1))

        return carry

    lax.fori_loop(0, heads + 1, turn, 0)

    def drain(h):
        @pl.when(sends_far)
        def _():
            far_copy(h).wait_send()

        @pl.when(has_far)
        def _():
            @pl.when(core == 1)
            def _():
                share_far(h).wait_send()

        @pl.when(jnp.logical_or(odd == 0, jnp.logical_and(has_far, h < last)))
        def _():
            near_copy(h).wait_send()

        @pl.when(has_near)
        def _():
            share_near(h).wait_send()

        @pl.when(core == 0)
        def _():
            share_own(h).wait_send()

    each_head(drain)

    @pl.when(passes)
    def _():
        pass_copy().wait_send()
        half_pass().wait_send()

    @pl.when(onward)
    def _():
        onward_copy().wait_send()
        half_onward().wait_send()

    @pl.when(jnp.logical_and(has_far, odd == 1))
    def _():
        near_half().wait_send()


def solution(mesh):
    n = mesh.shape["blk"]

    def per_device(queries, keys, values, doc_start):
        rows, columns = queries.shape
        heads = keys.shape[1] // HD
        span = (HOPS + 1) * rows
        remote_sems = [pltpu.SemaphoreType.DMA((heads,)) for _ in range(10)]
        return pl.pallas_call(
            functools.partial(kernel, n),
            out_shape=pltpu.VMEM((rows, columns), jnp.bfloat16),
            in_specs=[pl.BlockSpec(memory_space=pl.ANY)] * 3
            + [pl.BlockSpec(memory_space=pltpu.VMEM)],
            out_specs=pl.BlockSpec(memory_space=pltpu.VMEM),
            scratch_shapes=[
                pltpu.VMEM((rows, columns), jnp.bfloat16),
                pltpu.VMEM((heads, 2, (HOPS + 2) * rows, HD), jnp.bfloat16),
                pltpu.VMEM((2, rows, HD), jnp.bfloat16),
                pltpu.VMEM((rows, HD), jnp.bfloat16),
                pltpu.VMEM((rows, span), jnp.float32),
                pltpu.SemaphoreType.DMA,
                pltpu.SemaphoreType.DMA((2, heads)),
                pltpu.SemaphoreType.DMA((6,)),
            ]
            + [pltpu.SemaphoreType.DMA] * 4
            + remote_sems,
            compiler_params=pltpu.CompilerParams(collective_id=0, has_side_effects=True),
        )(queries, keys, values, doc_start.reshape(1, rows))

    return jax.shard_map(
        per_device,
        mesh=mesh,
        in_specs=(P("blk", None), P("blk", None), P("blk", None), P("blk")),
        out_specs=P("blk", None),
        check_vma=False,
    )
```

```python
import functools

import jax
import jax.numpy as jnp
from jax import lax
from jax.experimental import pallas as pl
from jax.experimental.pallas import tpu as pltpu
from jax.sharding import PartitionSpec as P

HD = 256
HOPS = 4
NEGATIVE = -1e30
FORWARD_AT = 2
MESH = pl.DeviceIdType.MESH


def kernel(
    n, q_hbm, k_hbm, v_hbm, doc_ref, out_ref,
    q_buf, kv, passing, passing_half, bias, q_sem, own_sem, half_sems, pass_send, pass_recv, onward_send, onward_recv,
    y_send, y_recv, x_send, x_recv, o_send, o_recv, p_send, p_recv, pp_send, pp_recv,
):
    rows = q_hbm.shape[0]
    heads = k_hbm.shape[1] // HD
    groups = q_hbm.shape[1] // k_hbm.shape[1]
    window = HOPS * rows
    span = window + rows
    wide = groups * HD

    me = lax.axis_index("blk")
    core = lax.rem(me, 2)
    chip = me // 2
    odd = lax.rem(chip, 2)
    partner = me + 1 - 2 * core
    beside = me + 2 - 4 * odd
    has_far = me >= 4
    has_near = jnp.logical_or(odd == 1, has_far)
    sends_far = me + 4 < n
    far_to = lax.rem(me + 4, n)

    def slot(number):
        return pl.ds(pl.multiple_of(number * rows, rows), rows)

    def own_copy(h, which):
        src = (k_hbm, v_hbm)[which]
        columns = pl.ds(pl.multiple_of(h * HD, HD), HD)
        return pltpu.make_async_copy(
            src.at[:, columns], kv.at[h, which, slot(4 + core), :], own_sem.at[which, h]
        )

    def remote(h, source, target, send, recv, device):
        return pltpu.make_async_remote_copy(
            src_ref=kv.at[h, :, slot(source), :],
            dst_ref=kv.at[h, :, slot(target), :],
            send_sem=send.at[h],
            recv_sem=recv.at[h],
            device_id=(device,),
            device_id_type=MESH,
        )

    def far_copy(h):
        return remote(h, 4 + core, core, y_send, y_recv, far_to)

    def near_copy(h):
        return remote(h, core + 4 * (1 - odd), 2 + core, x_send, x_recv, beside)

    last = heads - 2

    def odd_order(i):
        return jnp.where(i >= last, 2 * heads - 3 - i, i)

    def order(i):
        return jnp.where(odd == 1, odd_order(i), i)

    def pass_copy():
        return pltpu.make_async_remote_copy(
            src_ref=kv.at[last, :, slot(4 + core), :],
            dst_ref=passing,
            send_sem=pass_send,
            recv_sem=pass_recv,
            device_id=(beside,),
            device_id_type=MESH,
        )

    def half_pass():
        return pltpu.make_async_remote_copy(
            src_ref=kv.at[heads - 1, 1, slot(4 + core), :],
            dst_ref=passing_half,
            send_sem=half_sems.at[0],
            recv_sem=half_sems.at[1],
            device_id=(beside,),
            device_id_type=MESH,
        )

    def half_onward():
        return pltpu.make_async_remote_copy(
            src_ref=passing_half,
            dst_ref=kv.at[heads - 1, 1, slot(2 + core), :],
            send_sem=half_sems.at[2],
            recv_sem=half_sems.at[3],
            device_id=(far_to,),
            device_id_type=MESH,
        )

    def near_half():
        return pltpu.make_async_remote_copy(
            src_ref=kv.at[heads - 1, 0, slot(core + 4 * (1 - odd)), :],
            dst_ref=kv.at[heads - 1, 0, slot(2 + core), :],
            send_sem=half_sems.at[4],
            recv_sem=half_sems.at[5],
            device_id=(beside,),
            device_id_type=MESH,
        )

    def onward_copy():
        return pltpu.make_async_remote_copy(
            src_ref=passing,
            dst_ref=kv.at[last, :, slot(2 + core), :],
            send_sem=onward_send,
            recv_sem=onward_recv,
            device_id=(far_to,),
            device_id_type=MESH,
        )

    def share_own(h):
        return remote(h, 4, 4, o_send, o_recv, partner)

    def share_near(h):
        return remote(h, 2 + core, 2 + core, p_send, p_recv, partner)

    def near_shared(h):
        return remote(h, 3 - core, 3 - core, p_send, p_recv, partner)

    def share_far(h):
        return remote(h, 1, 1, pp_send, pp_recv, partner)

    def each_head(body):
        def step(h, carry):
            body(h)
            return carry

        lax.fori_loop(0, heads, step, 0)

    barrier = pltpu.get_barrier_semaphore()

    def greet(device):
        pl.semaphore_signal(barrier, inc=1, device_id=(device,), device_id_type=MESH)

    @pl.when(sends_far)
    def _():
        greet(me + 4)

    @pl.when(has_far)
    def _():
        greet(me - 4)

    greet(beside)
    greet(partner)

    q_copy = pltpu.make_async_copy(q_hbm, q_buf, q_sem)

    def load(h):
        own_copy(h, 0).start()
        own_copy(h, 1).start()

    each_head(load)
    q_copy.start()

    pl.semaphore_wait(barrier, 2 + jnp.where(sends_far, 1, 0) + jnp.where(has_far, 1, 0))

    passes = jnp.logical_and(sends_far, odd == 1)
    onward = jnp.logical_and(sends_far, odd == 0)
    takes = jnp.logical_and(has_far, odd == 0)

    def own_copy_wait(h):
        own_copy(h, 0).wait()
        own_copy(h, 1).wait()

    each_head(own_copy_wait)

    def send(i):
        h, near_head = order(i), odd_order(i)


        @pl.when(sends_far)
        def _():
            far_copy(h).start()

        @pl.when(odd == 0)
        def _():
            near_copy(near_head).start()

        @pl.when(core == 0)
        def _():
            share_own(h).start()

    each_head(send)

    @pl.when(passes)
    def _():
        pass_copy().start()
        half_pass().start()

    @pl.when(me < 4)
    def _():
        def clear(h):
            kv[h, :, 0 : 2 * rows, :] = jnp.zeros((2, 2 * rows, HD), kv.dtype)

        each_head(clear)

    @pl.when(me < 2)
    def _():
        def clear(h):
            kv[h, :, 2 * rows : 4 * rows, :] = jnp.zeros((2, 2 * rows, HD), kv.dtype)

        each_head(clear)

    square_row = lax.broadcasted_iota(jnp.int32, (rows, rows), 0)
    square_col = lax.broadcasted_iota(jnp.int32, (rows, rows), 1)
    spread = jnp.broadcast_to(doc_ref[...], (rows, rows)).astype(jnp.float32)
    starts = jnp.sum(jnp.where(square_row == square_col, spread, 0.0), axis=1, keepdims=True)
    starts = starts.astype(jnp.int32)
    q_pos = me * rows + lax.broadcasted_iota(jnp.int32, (rows, span), 0)
    k_pos = (me - HOPS) * rows + lax.broadcasted_iota(jnp.int32, (rows, span), 1)
    allowed = (k_pos <= q_pos) & (q_pos - k_pos < window) & (k_pos >= starts)
    bias[...] = jnp.where(allowed, 0.0, NEGATIVE)
    q_copy.wait()

    def relay(h):
        @pl.when(has_far)
        def _():
            far_copy(h).wait_recv()

            @pl.when(jnp.logical_and(odd == 1, h < last))
            def _():
                near_copy(h).start()

            @pl.when(jnp.logical_and(odd == 1, h > last))
            def _():
                near_half().start()

            @pl.when(core == 1)
            def _():
                share_far(h).start()

        @pl.when(has_near)
        def _():
            by_way = jnp.logical_and(takes, h == last)

            @pl.when(by_way)
            def _():
                onward_copy().wait_recv()

            by_halves = jnp.logical_and(takes, h > last)

            @pl.when(by_halves)
            def _():
                near_half().wait_recv()
                half_onward().wait_recv()

            @pl.when(jnp.logical_not(jnp.logical_or(by_way, by_halves)))
            def _():
                near_copy(h).wait_recv()

            share_near(h).start()

    def attend(h):
        @pl.when(has_near)
        def _():
            near_shared(h).wait_recv()

        @pl.when(jnp.logical_and(has_far, core == 0))
        def _():
            share_far(h).wait_recv()

        @pl.when(core == 1)
        def _():
            share_own(h).wait_recv()

        columns = pl.ds(pl.multiple_of(h * wide, wide), wide)
        query = q_buf[:, columns]
        query = jnp.concatenate(
            [query[:, g * HD : (g + 1) * HD] for g in range(groups)], axis=0
        )
        reach = pl.ds(pl.multiple_of(core * rows, rows), span)
        scores = lax.dot_general(
            query, kv[h, 0, reach, :], (((1,), (1,)), ((), ())),
            preferred_element_type=jnp.float32,
        ) * 0.0625
        hidden = jnp.concatenate([bias[...]] * groups, axis=0) < 0
        scores = jnp.where(hidden, NEGATIVE, scores)
        top = jnp.max(scores, axis=1, keepdims=True)
        expo = jnp.exp(scores - top)
        total = jnp.sum(expo, axis=1, keepdims=True)
        mixed = jnp.dot(
            expo.astype(jnp.bfloat16), kv[h, 1, reach, :],
            preferred_element_type=jnp.float32,
        )
        mixed = (mixed * (1.0 / total)).astype(out_ref.dtype)
        out_ref[:, columns] = jnp.concatenate(
            [mixed[g * rows : (g + 1) * rows] for g in range(groups)], axis=1
        )

    def turn(h, carry):
        @pl.when(jnp.logical_and(onward, h == FORWARD_AT))
        def _():
            pass_copy().wait_recv()
            onward_copy().start()
            half_pass().wait_recv()
            half_onward().start()

        @pl.when(h < heads)
        def _():
            relay(order(h))

        @pl.when(h >= 2)
        def _():
            attend(order(h - 2))

        return carry

    lax.fori_loop(0, heads + 2, turn, 0)

    def drain(h):
        @pl.when(sends_far)
        def _():
            far_copy(h).wait_send()

        @pl.when(has_far)
        def _():
            @pl.when(core == 1)
            def _():
                share_far(h).wait_send()

        @pl.when(jnp.logical_or(odd == 0, jnp.logical_and(has_far, h < last)))
        def _():
            near_copy(h).wait_send()

        @pl.when(has_near)
        def _():
            share_near(h).wait_send()

        @pl.when(core == 0)
        def _():
            share_own(h).wait_send()

    each_head(drain)

    @pl.when(passes)
    def _():
        pass_copy().wait_send()
        half_pass().wait_send()

    @pl.when(onward)
    def _():
        onward_copy().wait_send()
        half_onward().wait_send()

    @pl.when(jnp.logical_and(has_far, odd == 1))
    def _():
        near_half().wait_send()


def solution(mesh):
    n = mesh.shape["blk"]

    def per_device(queries, keys, values, doc_start):
        rows, columns = queries.shape
        heads = keys.shape[1] // HD
        span = (HOPS + 1) * rows
        remote_sems = [pltpu.SemaphoreType.DMA((heads,)) for _ in range(10)]
        return pl.pallas_call(
            functools.partial(kernel, n),
            out_shape=pltpu.VMEM((rows, columns), jnp.bfloat16),
            in_specs=[pl.BlockSpec(memory_space=pl.ANY)] * 3
            + [pl.BlockSpec(memory_space=pltpu.VMEM)],
            out_specs=pl.BlockSpec(memory_space=pltpu.VMEM),
            scratch_shapes=[
                pltpu.VMEM((rows, columns), jnp.bfloat16),
                pltpu.VMEM((heads, 2, (HOPS + 2) * rows, HD), jnp.bfloat16),
                pltpu.VMEM((2, rows, HD), jnp.bfloat16),
                pltpu.VMEM((rows, HD), jnp.bfloat16),
                pltpu.VMEM((rows, span), jnp.float32),
                pltpu.SemaphoreType.DMA,
                pltpu.SemaphoreType.DMA((2, heads)),
                pltpu.SemaphoreType.DMA((6,)),
            ]
            + [pltpu.SemaphoreType.DMA] * 4
            + remote_sems,
            compiler_params=pltpu.CompilerParams(collective_id=0, has_side_effects=True),
        )(queries, keys, values, doc_start.reshape(1, rows))

    return jax.shard_map(
        per_device,
        mesh=mesh,
        in_specs=(P("blk", None), P("blk", None), P("blk", None), P("blk")),
        out_specs=P("blk", None),
        check_vma=False,
    )
```
